32 devices in a mesh: zero: 8 (over z, x), width: 4 (over y, core).
Axes of the slice: x: 2, y: 2, z: 4, core: 2. Of those that a mesh axis runs over, the one named last changes fastest.
Arguments:
- weight_up: bfloat16 [12288, 49152], P('zero', 'width'), may hold values from -0.078125 to 0.078125
- low_up: bfloat16 [12288, 64], P('zero'), may hold values from -0.0546875 to 0.0546875
- high_up: bfloat16 [64, 49152], P(None, 'width'), may hold values from -0.75 to 0.75
- norm_train: float32 [12288], P(('zero', 'width')), may hold values from 0.25 to 1.75
- norm_step: float32 [12288], P(('zero', 'width')), may hold values from -0.3 to 0.3
Outputs:
- ready_up: bfloat16 [12288, 49152], P(None, ('width', 'zero'))
- scale_up: float32 [49152], P(('width', 'zero'))
- serve_norm: bfloat16 [12288], replicated
The draws below stay inside these ranges and needn't reach their ends.
All inputs are finite; a program needn't handle non-finite values. Where the reference program divides by a largest or mean magnitude, that divisor is 1e-20 or more.
Results may differ from the reference program's by a relative error of at most 0.001.
Values may be sent and summed in bfloat16 or wider, within the bound.
A program may use at most 192 MiB of HBM per device.

```python
import jax
import jax.numpy as jnp

D_MODEL = 12288
D_INNER = 49152
RANK = 64


def with_spikes(array, key, source, target, blocks, factor):
    def block_of(axis_at):
        return (jnp.arange(array.shape[axis_at]) // (array.shape[axis_at] // blocks)).reshape((-1,) + (1,) * (array.ndim - 1 - axis_at))

    one_side = jax.random.permutation(key, blocks)[block_of(target)]
    far = (block_of(target) + blocks // 2) % blocks
    return jnp.where((block_of(source) == one_side) | (block_of(source) == far), factor * array, array)


def level_of(own_key, dims, shards, low, top_value):
    factor_of, own = 1.0, jax.random.fold_in(own_key, 6)
    for position, blocks in shards:
        draws = jnp.exp(jax.random.uniform(jax.random.fold_in(own, position), (blocks,), jnp.float32, low / len(shards), top_value / len(shards)))
        factor_of = factor_of * jnp.repeat(draws, dims[position] // blocks).reshape([-1 if axis == position else 1 for axis in range(len(dims))])
    return factor_of


def scatter_about(stream_key, shape, spread, most, shards=(), dtype=jnp.bfloat16):
    level = level_of(stream_key, shape, shards, -0.22, 0.18) if shards else 1.0
    entries = jax.random.normal(stream_key, shape, jnp.float32) * spread * level
    return jnp.minimum(jnp.maximum(entries, -most), most).astype(dtype)


def bell_draw_with(key, extent, width, reach, split, heavy, dtype=jnp.bfloat16):
    result = width * jax.random.normal(key, extent, jnp.float32)
    if split:
        result = result * level_of(key, extent, split, -0.22, 0.18)
    return jnp.clip(with_spikes(result, jax.random.fold_in(key, 3), *heavy), -reach, reach).astype(dtype)


def setup_inputs(seed: int = 0) -> dict:
    splits = jax.random.split(jax.random.key(seed), 6)
    return {
        "weight_up": bell_draw_with(splits[0], (D_MODEL, D_INNER), D_MODEL ** -0.5, 0.078125, ((0, 8), (1, 4)), (0, 1, 8, 2.0)),
        "low_up": scatter_about(splits[1], (D_MODEL, RANK), D_MODEL ** -0.5, 0.0546875, ((0, 8),)),
        "high_up": scatter_about(splits[2], (RANK, D_INNER), RANK ** -0.5, 0.75, ((1, 4),)),
        "norm_train": jnp.clip(1.0 + 0.15 * jax.random.normal(splits[3], (D_MODEL,), jnp.float32), 0.25, 1.75),
        "norm_step": jnp.clip(jax.random.uniform(splits[4], (D_MODEL,), jnp.float32, -0.3, 0.3) * level_of(splits[4], (D_MODEL,), ((0, 32),), -0.4, 0.0), -0.3, 0.3),
    }


mix_rate = 2.0


def reference(weight_up, low_up, high_up, norm_train, norm_step):
    latest_up = weight_up.astype(jnp.float32) + mix_rate * jnp.dot(low_up, high_up, preferred_element_type=jnp.float32)
    scale_up = jnp.max(jnp.abs(latest_up), axis=0)
    ready_up = (latest_up / scale_up).astype(jnp.bfloat16)
    serve_norm = (norm_train + norm_step).astype(jnp.bfloat16)
    return ready_up, scale_up, serve_norm
```

```python
import functools

import jax
import jax.numpy as jnp
from jax import lax
from jax.experimental import pallas as pl
from jax.experimental.pallas import tpu as pltpu
from jax.sharding import PartitionSpec as P


mix_rate = 2.0


def latest(weight_ref, low_ref, high_ref):
    return weight_ref[...].astype(jnp.float32) + jnp.dot(
        low_ref[...], high_ref[...], preferred_element_type=jnp.float32
    )


def top_kernel(place_ref, weight_ref, low_ref, high_ref, before_ref, top_ref):
    @pl.when(pl.program_id(0) == 0)
    def _():
        top_ref[...] = before_ref[...]

    top = jnp.max(jnp.abs(latest(weight_ref, low_ref, high_ref)), axis=0, keepdims=True)
    top_ref[...] = jnp.maximum(top_ref[...], top)


def ready_kernel(tiles, n, place_ref, *refs):
    blocks, (low_ref, high_ref, scale_ref, ready_ref) = refs[:n], refs[n:]
    for b in range(n):

        @pl.when(pl.program_id(0) // tiles == b)
        def _():
            ready_ref[...] = (
                latest(blocks[b], low_ref, high_ref) * (1.0 / scale_ref[...])
            ).astype(jnp.bfloat16)


def column_top(place, block, low_all, high, before, tile):
    rows, cols = block.shape
    rank = low_all.shape[1]
    tiles = rows // tile
    return pl.pallas_call(
        top_kernel,
        grid_spec=pltpu.PrefetchScalarGridSpec(
            num_scalar_prefetch=1,
            grid=(tiles,),
            in_specs=[
                pl.BlockSpec((tile, cols), lambda i, p: (i, 0)),
                pl.BlockSpec((tile, rank), lambda i, p: (p[0] * tiles + i, 0)),
                pl.BlockSpec((rank, cols), lambda i, p: (0, 0)),
                pl.BlockSpec((1, cols), lambda i, p: (0, 0)),
            ],
            out_specs=pl.BlockSpec((1, cols), lambda i, p: (0, 0)),
        ),
        out_shape=jax.ShapeDtypeStruct((1, cols), jnp.float32),
        cost_estimate=pl.CostEstimate(
            flops=2 * rows * cols * rank, bytes_accessed=2 * rows * cols, transcendentals=0
        ),
        name="column_top",
    )(place.reshape(1), block, low_all, high, before)


def place_ready(places, blocks, low_all, high, scale, tile):
    n = len(blocks)
    rows, cols = blocks[0].shape
    rank = low_all.shape[1]
    tiles = rows // tile

    def own_tile(b):
        return lambda s, p: (jnp.clip(s - b * tiles, 0, tiles - 1), 0)

    def row_tile(s, p):
        return (p[s // tiles] * tiles + s % tiles, 0)

    return pl.pallas_call(
        functools.partial(ready_kernel, tiles, n),
        grid_spec=pltpu.PrefetchScalarGridSpec(
            num_scalar_prefetch=1,
            grid=(n * tiles,),
            in_specs=[pl.BlockSpec((tile, cols), own_tile(b)) for b in range(n)]
            + [
                pl.BlockSpec((tile, rank), row_tile),
                pl.BlockSpec((rank, cols), lambda s, p: (0, 0)),
                pl.BlockSpec((1, cols), lambda s, p: (0, 0)),
            ],
            out_specs=pl.BlockSpec((tile, cols), row_tile),
        ),
        out_shape=jax.ShapeDtypeStruct((n * rows, cols), jnp.bfloat16),
        cost_estimate=pl.CostEstimate(
            flops=2 * n * rows * cols * rank,
            bytes_accessed=4 * n * rows * cols,
            transcendentals=0,
        ),
        name="place_ready",
    )(jnp.stack(places), *blocks, low_all, high, scale)


def by_permutes(n, wide, weight_up, low_up, high_up, norm_train, norm_step):
    me = lax.axis_index("zero")
    rows, all_cols = weight_up.shape
    cols, rank = all_cols // n, low_up.shape[1]
    share = rows // wide
    norm = (norm_train + norm_step).astype(jnp.bfloat16)
    part = lax.dynamic_slice_in_dim(low_up, lax.axis_index("width") * share, share)
    sent = jnp.concatenate([part.reshape(-1), norm])
    gathered = lax.all_gather(sent, ("zero", "width"), axis=0, tiled=False)
    low_all = gathered[:, : share * rank].reshape(n * rows, rank)
    serve_norm = gathered[:, share * rank :].reshape(-1)
    high = lax.dynamic_slice_in_dim(high_up, me * cols, cols, axis=1) * jnp.bfloat16(mix_rate)

    blocks, places = [], []
    for k in range(1, n):
        target = lax.rem(me + k, n)
        block = lax.dynamic_slice_in_dim(weight_up, target * cols, cols, axis=1)
        block, weight_up = lax.optimization_barrier((block, weight_up))
        blocks.append(lax.ppermute(block, "zero", [(i, (i + k) % n) for i in range(n)]))
        places.append(lax.rem(me + n - k, n))
    blocks.insert(0, lax.dynamic_slice_in_dim(weight_up, me * cols, cols, axis=1))
    places.insert(0, me)
    tile = rows // 6 if rows % 96 == 0 else rows // 4
    scale = jnp.zeros((1, cols), jnp.float32)
    for b, p in zip(blocks, places):
        scale = column_top(p, b, low_all, high, scale, tile)
    ready = place_ready(places, blocks, low_all, high, scale, tile)
    return ready, scale.reshape(-1), serve_norm


def by_exchange(weight_up, low_up, high_up, norm_train, norm_step):
    latest_up = weight_up.astype(jnp.float32) + mix_rate * jnp.dot(
        low_up, high_up, preferred_element_type=jnp.float32
    )
    scale_up = lax.pmax(jnp.max(jnp.abs(latest_up), axis=0), "zero")
    narrow_up = (latest_up / scale_up).astype(jnp.bfloat16)
    ready_up = lax.all_to_all(narrow_up, "zero", split_axis=1, concat_axis=0, tiled=True)
    place = lax.axis_index("zero")
    scale_up = lax.dynamic_slice_in_dim(scale_up, place * ready_up.shape[1], ready_up.shape[1])
    serve_norm = lax.all_gather(
        (norm_train + norm_step).astype(jnp.bfloat16), ("zero", "width"), axis=0, tiled=True
    )
    return (ready_up, scale_up, serve_norm)


def solution(mesh):
    n, wide = mesh.shape["zero"], mesh.shape["width"]

    def shards(weight_up, low_up, high_up, norm_train, norm_step):
        rows, all_cols = weight_up.shape
        given = (weight_up, low_up, high_up, norm_train, norm_step)
        if n <= 16 and all_cols % (n * 128) == 0 and rows % (64 * wide) == 0:
            return by_permutes(n, wide, *given)
        return by_exchange(*given)

    return jax.shard_map(
        shards,
        mesh=mesh,
        in_specs=(
            P("zero", "width"),
            P("zero", None),
            P(None, "width"),
            P(("zero", "width")),
            P(("zero", "width")),
        ),
        out_specs=(P(None, ("width", "zero")), P(("width", "zero")), P()),
        check_vma=False,
    )
```
